128 devices in a mesh: bank: 4 (over y), zero: 32 (over z, x, core).
Axes of the slice: x: 4, y: 4, z: 4, core: 2. Of those that a mesh axis runs over, the one named last changes fastest.
Arguments:
- train_gate: float32 [64, 2048, 1024], P('bank', 'zero'), may hold values from -0.25 to 0.25
- train_up: float32 [64, 2048, 1024], P('bank', 'zero'), may hold values from -0.25 to 0.25
- train_down: float32 [64, 1024, 2048], P('bank', None, 'zero'), may hold values from -0.375 to 0.375
- router_weight: float32 [2048, 64], P('zero', 'bank'), may hold values from -0.125 to 0.125
- router_gain: float32 [2048], P('zero'), may hold values from 0.25 to 1.75
Outputs:
- ready_gate: bfloat16 [64, 2048, 1024], P('bank', None, 'zero')
- ready_up: bfloat16 [64, 2048, 1024], P('bank', None, 'zero')
- ready_down: bfloat16 [64, 1024, 2048], P('bank', 'zero')
- scale_gate: float32 [64, 1024], P('bank', 'zero')
- scale_up: float32 [64, 1024], P('bank', 'zero')
- scale_down: float32 [64, 1024], P('bank', 'zero')
- serve_router: bfloat16 [2048, 64], replicated
The draws below stay inside these ranges and needn't reach their ends.
All inputs are finite; a program needn't handle non-finite values.
Results may differ from the reference program's by a relative error of at most 0.001.
Values may be sent and summed in bfloat16 or wider, within the bound.
A program may use at most 128 MiB of HBM per device.

```python
import jax
import jax.numpy as jnp
from jax import lax

EXPERTS = 64
D_MODEL = 2048
D_EXPERT = 1024


def spiked(result, rng, source, target, blocks, factor):
    owner, partner = [(jnp.arange(result.shape[axis_at]) // (result.shape[axis_at] // blocks)).reshape([-1 if axis == axis_at else 1 for axis in range(result.ndim)]) for axis_at in (source, target)]
    chosen = jax.random.permutation(rng, blocks)[partner]
    strong = (owner == chosen) | (owner == (partner + blocks // 2) % blocks)
    return jnp.where(strong, factor * result, result)


def level_of(rng, shape, shards, least, top_value):
    factor_of, own = 1.0, jax.random.fold_in(rng, 6)
    for axis_at, shards_of in shards:
        heights = jnp.exp(jax.random.uniform(jax.random.fold_in(own, axis_at), (shards_of,), jnp.float32, least / len(shards), top_value / len(shards)))
        factor_of = factor_of * jnp.repeat(heights, shape[axis_at] // shards_of).reshape([-1 if axis == axis_at else 1 for axis in range(len(shape))])
    return factor_of


def scatter_about(own_key, shape, spread, limit, split=(), dtype=jnp.bfloat16):
    array = spread * jax.random.normal(own_key, shape, jnp.float32)
    if split:
        array = array * level_of(own_key, shape, split, -0.22, 0.18)
    return jnp.clip(array, -limit, limit).astype(dtype)


def noise_with(stream_key, extent, scale, reach, split, heavy, kind=jnp.bfloat16):
    drawn = scale * jax.random.normal(stream_key, extent, jnp.float32)
    if split:
        drawn = drawn * level_of(stream_key, extent, split, -0.22, 0.18)
    return jnp.clip(spiked(drawn, jax.random.fold_in(stream_key, 3), *heavy), -reach, reach).astype(kind)


def setup_inputs(seed: int = 0) -> dict:
    streams_of = jax.random.split(jax.random.key(seed), 6)
    return {
        "train_gate": noise_with(streams_of[0], (EXPERTS, D_MODEL, D_EXPERT), D_MODEL ** -0.5, 0.25, ((0, 4), (1, 32)), (1, 2, 32, 2.75), jnp.float32),
        "train_up": noise_with(streams_of[1], (EXPERTS, D_MODEL, D_EXPERT), D_MODEL ** -0.5, 0.25, ((0, 4), (1, 32)), (1, 2, 32, 2.75), jnp.float32),
        "train_down": noise_with(streams_of[2], (EXPERTS, D_EXPERT, D_MODEL), D_EXPERT ** -0.5, 0.375, ((0, 4), (2, 32)), (2, 1, 32, 2.75), jnp.float32),
        "router_weight": scatter_about(streams_of[3], (D_MODEL, EXPERTS), D_MODEL ** -0.5, 0.125, ((0, 32), (1, 4)), jnp.float32),
        "router_gain": jnp.clip(1.0 + 0.15 * jax.random.normal(streams_of[4], (D_MODEL,), jnp.float32), 0.25, 1.75),
    }


def reference(train_gate, train_up, train_down, router_weight, router_gain):
    scale_gate = jnp.sqrt(lax.optimization_barrier(jnp.sum(train_gate * train_gate, axis=1)))
    ready_gate = (train_gate / jnp.expand_dims(scale_gate, 1)).astype(jnp.bfloat16)
    scale_up = jnp.sqrt(lax.optimization_barrier(jnp.sum(train_up * train_up, axis=1)))
    ready_up = (train_up / jnp.expand_dims(scale_up, 1)).astype(jnp.bfloat16)
    scale_down = jnp.sqrt(lax.optimization_barrier(jnp.sum(train_down * train_down, axis=2)))
    ready_down = (train_down / jnp.expand_dims(scale_down, 2)).astype(jnp.bfloat16)
    serve_router = (router_weight * router_gain[:, None]).astype(jnp.bfloat16)
    return (ready_gate, ready_up, ready_down, scale_gate, scale_up, scale_down, serve_router)
```

```python
import functools

import jax
import jax.numpy as jnp
from jax import lax
from jax.experimental import pallas as pl
from jax.experimental.pallas import tpu as pltpu
from jax.sharding import Mesh
from jax.sharding import PartitionSpec as P

ZERO = ("z", "x", "c")
MESH = pl.DeviceIdType.MESH
F32 = jnp.float32
BF16 = jnp.bfloat16
HALF = 8
SLOTS = 3 * HALF
PAIRS = SLOTS // 2
LAG = 2
GROUPS = ((0, 2), (2, 6), (8, 8), (16, 8))


def kernel(
    gate, up, down, weight, gain, out, scales, router,
    full, turned, relay, xsum, zsum, scale, other, inverse, swap, part,
    load_sem, core_send, core_recv, xs_send, xs_recv, zs_send, zs_recv,
    one_send, one_recv, two_send, two_recv, sc_send, sc_recv, rt_send, rt_recv,
):
    b, z, x, c = (lax.axis_index(n) for n in ("b", "z", "x", "c"))
    oc = 1 - c

    def xdev(k):
        return {"x": lax.rem(x + k, 4)}

    def zdev(k):
        return {"z": lax.rem(z + k, 4)}

    def remote(src, dst, send, recv, dev):
        pltpu.make_async_remote_copy(
            src_ref=src, dst_ref=dst, send_sem=send, recv_sem=recv, device_id=dev, device_id_type=MESH
        ).start()

    def wait_bytes(ref, sem):
        pltpu.make_async_copy(ref, ref, sem).wait()

    sources = (gate, up, down)
    mine = pl.ds(pl.multiple_of(c * 64, 64), 64)

    for k, (first, n) in enumerate(GROUPS):
        src = sources[first // HALF]
        pltpu.make_async_copy(
            src.at[pl.ds(c * HALF + first % HALF, n)], full.at[pl.ds(first, n), mine], load_sem.at[k]
        ).start()

    barrier = pltpu.get_barrier_semaphore()
    peers = [{"c": oc}]
    for k in (1, 2, 3):
        peers += [xdev(k), zdev(k), {**xdev(k), "c": oc}, {**zdev(k), "c": oc}, {"b": lax.rem(b + k, 4)}]
    for dev in peers:
        pl.semaphore_signal(barrier, inc=1, device_id=dev, device_id_type=MESH)

    product = weight[...] * gain[...]
    swap[0] = jnp.concatenate([product, product], axis=1).reshape(2, HALF, 128)
    pl.semaphore_wait(barrier, len(peers))

    for k, (first, n) in enumerate(GROUPS):
        src = sources[first // HALF]
        remote(
            src.at[pl.ds(oc * HALF + first % HALF, n)], full.at[pl.ds(first, n), mine],
            core_send.at[k], core_recv.at[k], {"c": oc},
        )
    remote(swap.at[0, oc], swap.at[1, 0], rt_send.at[0], rt_recv.at[0], {"c": oc})

    def sums(k):
        first, n = GROUPS[k]
        pltpu.make_async_copy(
            gate.at[pl.ds(0, n)], full.at[pl.ds(first, n), mine], load_sem.at[k]
        ).wait()
        wait_bytes(full.at[pl.ds(first, n), mine], core_recv.at[k])

        def one(q, carry):
            rows = full[q]
            xsum[x, q] = jnp.sum(rows * rows, axis=0, keepdims=True)
            return carry

        lax.fori_loop(first, first + n, one, 0)
        at = pl.ds(first, n)
        for j in (1, 2, 3):
            remote(xsum.at[x, at], xsum.at[x, at], xs_send.at[k], xs_recv.at[k], xdev(j))

    def fold_x(k):
        first, n = GROUPS[k]
        at = pl.ds(first, n)
        wait_bytes(xsum.at[pl.ds(0, 3), at], xs_recv.at[k])
        zsum[z, at] = (xsum[0, at] + xsum[1, at]) + (xsum[2, at] + xsum[3, at])
        for j in (1, 2, 3):
            remote(zsum.at[z, at], zsum.at[z, at], zs_send.at[k], zs_recv.at[k], zdev(j))

    def fold_z(k):
        first, n = GROUPS[k]
        at = pl.ds(first, n)
        wait_bytes(zsum.at[pl.ds(0, 3), at], zs_recv.at[k])
        root = jnp.sqrt((zsum[0, at] + zsum[1, at]) + (zsum[2, at] + zsum[3, at]))
        scale[at] = root
        inverse[at] = 1.0 / root

    def turn(q):
        for j in range(8):
            lanes = slice(j * 128, (j + 1) * 128)
            block = (full[q, :, lanes] * inverse[q, :, lanes]).astype(BF16)
            turned[q, j // 2, (j % 2) * 2 : (j % 2) * 2 + 2] = block.T.reshape(2, 64, 128)

    xlane = pl.ds(pl.multiple_of(x * 128, 128), 128)
    zlane = pl.ds(pl.multiple_of(z * 128, 128), 128)
    zwide = pl.ds(pl.multiple_of(z * 512, 512), 512)

    def first_hop(p):
        qa, qb = 2 * p, 2 * p + 1
        turn(qa)
        turn(qb)
        for j in (1, 2, 3):
            to = lax.rem(x + j, 4)
            remote(turned.at[qa, :, to], relay.at[qa, :, :, xlane], one_send, one_recv.at[qa], xdev(j))
            to = lax.rem(z + j, 4)
            remote(turned.at[qb, to], relay.at[qb, :, :, zlane], one_send, one_recv.at[qb], zdev(j))
        relay[qa, :, :, xlane] = turned[qa, :, x]
        relay[qb, :, :, zlane] = turned[qb, z]

    def second_hop(p):
        qa, qb = 2 * p, 2 * p + 1
        ea = (qa // HALF) * 16 + c * HALF + lax.rem(qa, HALF)
        eb = ea + 1
        wait_bytes(relay.at[qa, pl.ds(0, 3)], one_recv.at[qa])
        wait_bytes(relay.at[qb, pl.ds(0, 3)], one_recv.at[qb])
        for j in (1, 2, 3, 0):
            tz, tx = lax.rem(z + j, 4), lax.rem(x + j, 4)
            for cc in (c, oc):
                rows = pl.ds(pl.multiple_of(cc * 32, 32), 32)
                if j == 0 and cc is c:
                    out[ea, :, zwide] = relay[qa, z, rows]
                    for s in range(4):
                        at = pl.ds(pl.multiple_of(s * 512 + x * 128, 128), 128)
                        out[eb, :, at] = relay[qb, x, rows, s * 128 : (s + 1) * 128]
                    continue
                other_core = {} if cc is c else {"c": oc}
                remote(
                    relay.at[qa, tz, rows], out.at[ea, :, zwide], two_send, two_recv,
                    {**zdev(j), **other_core} if j else other_core,
                )
                for s in range(4):
                    at = pl.ds(pl.multiple_of(s * 512 + x * 128, 128), 128)
                    remote(
                        relay.at[qb, tx, rows, pl.ds(s * 128, 128)], out.at[eb, :, at], two_send, two_recv,
                        {**xdev(j), **other_core} if j else other_core,
                    )

    place = b * 2 + c
    chip = pl.ds(pl.multiple_of((z * 4 + x) * 128, 128), 128)

    def router_start():
        wait_bytes(swap.at[1, 0], rt_recv.at[0])
        lane = lax.broadcasted_iota(jnp.int32, (HALF, 128), 1)
        own = (lane < 64) == (c == 0)
        part[...] = jnp.where(own, swap[0, c], swap[1, 0]).astype(BF16)
        router[place, :, chip] = part[...]
        for j in (1, 2, 3):
            remote(part, router.at[place, :, chip], rt_send.at[1], rt_recv.at[1], xdev(j))

    def router_z():
        wait_bytes(router.at[place, :, pl.ds(0, 384)], rt_recv.at[1])
        for j in (1, 2, 3):
            remote(
                router.at[place, :, zwide], router.at[place, :, zwide], rt_send.at[2], rt_recv.at[2], zdev(j)
            )

    def router_y():
        wait_bytes(router.at[place, :, pl.ds(0, 1536)], rt_recv.at[2])
        for j in (1, 2, 3):
            remote(
                router.at[place], router.at[place], rt_send.at[3], rt_recv.at[3], {"b": lax.rem(b + j, 4)}
            )

    def router_core():
        wait_bytes(router.at[pl.ds(0, 3)], rt_recv.at[3])
        for j in range(4):
            remote(router.at[2 * j + c], router.at[2 * j + c], rt_send.at[4], rt_recv.at[4], {"c": oc})

    sums(0)
    sums(1)
    fold_x(0)
    sums(2)
    fold_z(0)
    first_hop(0)
    fold_x(1)
    sums(3)
    fold_z(1)
    first_hop(1)
    fold_x(2)
    fold_x(3)
    router_start()
    first_hop(2)
    second_hop(0)
    fold_z(2)
    fold_z(3)
    remote(scale, other, sc_send, sc_recv, {"c": oc})
    router_z()

    def step(p, carry):
        first_hop(p)
        second_hop(p - LAG)
        return carry

    lax.fori_loop(3, 6, step, 0)
    router_y()
    lax.fori_loop(6, 9, step, 0)
    router_core()
    lax.fori_loop(9, PAIRS, step, 0)

    wait_bytes(scale, sc_recv)
    wait_bytes(scale, sc_send)
    index = (z * 4 + x) * 2 + c
    turn_by = lax.rem(4 - lax.rem(index, 4), 4) * 32
    column = pl.ds(pl.multiple_of((index // 4) * 128, 128), 128)

    def emit(q, carry):
        row = (q // HALF) * 16 + lax.rem(q, HALF)
        scales[row + c * HALF] = pltpu.roll(scale[q, :, column], turn_by, 1)
        scales[row + oc * HALF] = pltpu.roll(other[q, :, column], turn_by, 1)
        return carry

    lax.fori_loop(0, SLOTS, emit, 0)

    for p in range(PAIRS - LAG, PAIRS):
        second_hop(p)

    wait_bytes(router.at[pl.ds(0, 4)], rt_recv.at[4])
    wait_bytes(swap.at[1, 0], rt_send.at[0])
    wait_bytes(router.at[place, :, pl.ds(0, 384)], rt_send.at[1])
    wait_bytes(router.at[place, :, pl.ds(0, 1536)], rt_send.at[2])
    wait_bytes(router.at[pl.ds(0, 3)], rt_send.at[3])
    wait_bytes(router.at[pl.ds(0, 4)], rt_send.at[4])
    for k, (first, n) in enumerate(GROUPS):
        wait_bytes(full.at[pl.ds(first, n), mine], core_send.at[k])
        wait_bytes(xsum.at[pl.ds(0, 3), pl.ds(first, n)], xs_send.at[k])
        wait_bytes(zsum.at[pl.ds(0, 3), pl.ds(first, n)], zs_send.at[k])
    wait_bytes(turned.at[pl.ds(0, SLOTS * 3 // 4)], one_send)
    wait_bytes(out.at[pl.ds(0, 42)], two_send)
    wait_bytes(out.at[pl.ds(0, 42)], two_recv)


def body(train_gate, train_up, train_down, router_weight, router_gain):
    vmem = pl.BlockSpec(memory_space=pltpu.VMEM)
    anywhere = pl.BlockSpec(memory_space=pl.ANY)
    dma = pltpu.SemaphoreType.DMA
    groups = len(GROUPS)
    out, scales, router = pl.pallas_call(
        kernel,
        out_shape=(
            jax.ShapeDtypeStruct((48, 32, 2048), BF16),
            jax.ShapeDtypeStruct((48, 1, 128), F32),
            jax.ShapeDtypeStruct((8, 8, 2048), BF16),
        ),
        in_specs=[anywhere] * 3 + [vmem] * 2,
        out_specs=(vmem, vmem, vmem),
        scratch_shapes=[
            pltpu.VMEM((SLOTS, 128, 1024), F32),
            pltpu.VMEM((SLOTS, 4, 4, 64, 128), BF16),
            pltpu.VMEM((SLOTS, 4, 64, 512), BF16),
            pltpu.VMEM((4, SLOTS, 1, 1024), F32),
            pltpu.VMEM((4, SLOTS, 1, 1024), F32),
            pltpu.VMEM((SLOTS, 1, 1024), F32),
            pltpu.VMEM((SLOTS, 1, 1024), F32),
            pltpu.VMEM((SLOTS, 1, 1024), F32),
            pltpu.VMEM((2, 2, HALF, 128), F32),
            pltpu.VMEM((HALF, 128), BF16),
            dma((groups,)), dma((groups,)), dma((groups,)), dma((groups,)), dma((groups,)),
            dma((groups,)), dma((groups,)),
            dma, dma((SLOTS,)), dma, dma, dma, dma, dma((5,)), dma((5,)),
        ],
        compiler_params=pltpu.CompilerParams(
            collective_id=0, has_side_effects=True, vmem_limit_bytes=52 * 1024 * 1024
        ),
    )(
        train_gate,
        train_up,
        jnp.transpose(train_down, (0, 2, 1)),
        router_weight.T,
        router_gain.reshape(1, 64),
    )
    ready_gate, ready_up, ready_down = out[:16], out[16:32], out[32:]
    scale_gate, scale_up, scale_down = (scales[16 * t : 16 * t + 16, 0, :32] for t in range(3))
    return (
        jnp.transpose(ready_gate, (0, 2, 1)),
        jnp.transpose(ready_up, (0, 2, 1)),
        ready_down,
        scale_gate,
        scale_up,
        scale_down,
        router.reshape(64, 2048).T,
    )


def solution(mesh):
    split = Mesh(mesh.devices.reshape(mesh.shape["bank"], 4, 4, 2), ("b",) + ZERO)
    return jax.shard_map(
        body,
        mesh=split,
        in_specs=(P("b", ZERO, None), P("b", ZERO, None), P("b", None, ZERO), P(ZERO, "b"), P(ZERO)),
        out_specs=(
            P("b", None, ZERO),
            P("b", None, ZERO),
            P("b", ZERO, None),
            P("b", ZERO),
            P("b", ZERO),
            P("b", ZERO),
            P(),
        ),
        check_vma=False,
    )
```

```python
import functools

import jax
import jax.numpy as jnp
from jax import lax
from jax.experimental import pallas as pl
from jax.experimental.pallas import tpu as pltpu
from jax.sharding import Mesh
from jax.sharding import PartitionSpec as P

ZERO = ("z", "x", "c")
MESH = pl.DeviceIdType.MESH
F32 = jnp.float32
BF16 = jnp.bfloat16
HALF = 8
SLOTS = 3 * HALF
PAIRS = SLOTS // 2
LAG = 2
CHUNKS = ((0, 2), (2, 6), (8, 8), (16, 8))
ALONG_X = (2, 10)
ALONG_Z = (12, 12)


def kernel(
    gate, up, down, weight, gain, out, scales, router,
    full, half, turned, relay, own_sum, lent_sum, got_sum, pair_sum, stage_one, stage_two,
    scale, other, inverse, swap, part, weight_in, gain_in,
    load_sem, core_send, core_recv, sum_send, sum_recv,
    one_send, one_recv, two_send, two_recv, sc_send, sc_recv, rt_send, rt_recv,
):
    b, z, x, c = (lax.axis_index(n) for n in ("b", "z", "x", "c"))
    oc = 1 - c

    def xdev(k):
        return {"x": lax.rem(x + k, 4)}

    def zdev(k):
        return {"z": lax.rem(z + k, 4)}

    def remote(src, dst, send, recv, dev):
        pltpu.make_async_remote_copy(
            src_ref=src, dst_ref=dst, send_sem=send, recv_sem=recv, device_id=dev, device_id_type=MESH
        ).start()

    def wait_bytes(ref, sem):
        pltpu.make_async_copy(ref, ref, sem).wait()

    barrier = pltpu.get_barrier_semaphore()
    peers = [{"c": oc}]
    for k in (1, 2, 3):
        peers += [xdev(k), zdev(k), {**xdev(k), "c": oc}, {**zdev(k), "c": oc}, {"b": lax.rem(b + k, 4)}]
    for dev in peers:
        pl.semaphore_signal(barrier, inc=1, device_id=dev, device_id_type=MESH)

    sources = (gate, up, down)
    mine = pl.ds(pl.multiple_of(c * 64, 64), 64)

    loads = []
    for k, (first, n) in enumerate(CHUNKS):
        src, at = sources[first // HALF], pl.ds(first, n)
        loads.append((
            pltpu.make_async_copy(
                src.at[pl.ds(c * HALF + first % HALF, n)], full.at[at, mine], load_sem.at[2 * k]
            ),
            pltpu.make_async_copy(
                src.at[pl.ds(oc * HALF + first % HALF, n)], half.at[at], load_sem.at[2 * k + 1]
            ),
        ))
    loads.append((
        pltpu.make_async_copy(weight, weight_in, load_sem.at[2 * len(CHUNKS)]),
        pltpu.make_async_copy(gain, gain_in, load_sem.at[2 * len(CHUNKS) + 1]),
    ))
    for pair in loads:
        for copy in pair:
            copy.start()

    def own_sums(k):
        first, n = CHUNKS[k]
        for copy in loads[k]:
            copy.wait()

        def one(q, carry):
            rows = full[q, mine]
            own_sum[q] = jnp.sum(rows * rows, axis=0, keepdims=True)
            rows = half[q]
            lent_sum[q] = jnp.sum(rows * rows, axis=0, keepdims=True)
            return carry

        lax.fori_loop(first, first + n, one, 0)

    own_sums(0)
    lead = pl.ds(0, 2)
    pair_sum[x * 2 + c] = own_sum[lead]
    pl.semaphore_wait(barrier, len(peers))

    here = x * 2 + c
    for j in (1, 2, 3):
        remote(pair_sum.at[here], pair_sum.at[here], sum_send.at[0], sum_recv.at[0], xdev(j))
    for j in (1, 2, 3):
        remote(lent_sum.at[lead], pair_sum.at[here], sum_send.at[0], sum_recv.at[0], {**xdev(j), "c": oc})
    remote(lent_sum.at[lead], pair_sum.at[here], sum_send.at[0], sum_recv.at[0], {"c": oc})
    for k in range(1, len(CHUNKS)):
        own_sums(k)

    def lend(k):
        first, n = CHUNKS[k]
        at = pl.ds(first, n)
        remote(half.at[at], full.at[at, mine], core_send.at[k], core_recv.at[k], {"c": oc})

    rest = pl.ds(2, SLOTS - 2)
    remote(lent_sum.at[rest], got_sum.at[rest], sum_send.at[1], sum_recv.at[1], {"c": oc})
    for k in range(len(CHUNKS)):
        lend(k)

    for copy in loads[-1]:
        copy.wait()
    product = weight_in[...] * gain_in[...]
    swap[0] = jnp.concatenate([product, product], axis=1).reshape(2, HALF, 128)

    wait_bytes(pair_sum.at[pl.ds(0, 7)], sum_recv.at[0])
    total = [pair_sum[2 * k] + pair_sum[2 * k + 1] for k in range(4)]
    stage_two[z, lead] = (total[0] + total[1]) + (total[2] + total[3])
    for j in (1, 2, 3):
        remote(stage_two.at[z, lead], stage_two.at[z, lead], sum_send.at[2], sum_recv.at[2], zdev(j))

    wait_bytes(lent_sum.at[rest], sum_recv.at[1])
    plans = ((ALONG_X, x, xdev, z, zdev, 3, 5), (ALONG_Z, z, zdev, x, xdev, 4, 6))
    for (first, n), me, dev, _, _, sem, _ in plans:
        at = pl.ds(first, n)
        stage_one[me, at] = own_sum[at] + got_sum[at]
        for j in (1, 2, 3):
            remote(stage_one.at[me, at], stage_one.at[me, at], sum_send.at[sem], sum_recv.at[sem], dev(j))
    remote(swap.at[0, oc], swap.at[1, 0], rt_send.at[0], rt_recv.at[0], {"c": oc})

    def finish(at):
        root = jnp.sqrt((stage_two[0, at] + stage_two[1, at]) + (stage_two[2, at] + stage_two[3, at]))
        scale[at] = root
        inverse[at] = 1.0 / root

    def turn(q):
        for j in range(8):
            lanes = slice(j * 128, (j + 1) * 128)
            block = (full[q, :, lanes] * inverse[q, :, lanes]).astype(BF16)
            turned[q, j // 2, (j % 2) * 2 : (j % 2) * 2 + 2] = block.T.reshape(2, 64, 128)

    xlane = pl.ds(pl.multiple_of(x * 128, 128), 128)
    zlane = pl.ds(pl.multiple_of(z * 128, 128), 128)
    zwide = pl.ds(pl.multiple_of(z * 512, 512), 512)

    def first_hop(p):
        qa, qb = 2 * p, 2 * p + 1
        turn(qa)
        for j in (1, 2, 3):
            to = lax.rem(x + j, 4)
            remote(turned.at[qa, :, to], relay.at[qa, :, :, xlane], one_send, one_recv.at[qa], xdev(j))
        turn(qb)
        for j in (1, 2, 3):
            to = lax.rem(z + j, 4)
            remote(turned.at[qb, to], relay.at[qb, :, :, zlane], one_send, one_recv.at[qb], zdev(j))
        relay[qa, :, :, xlane] = turned[qa, :, x]
        relay[qb, :, :, zlane] = turned[qb, z]

    def second_hop(p):
        qa, qb = 2 * p, 2 * p + 1
        ea = (qa // HALF) * 16 + c * HALF + lax.rem(qa, HALF)
        eb = ea + 1
        wait_bytes(relay.at[qa, pl.ds(0, 3)], one_recv.at[qa])
        wait_bytes(relay.at[qb, pl.ds(0, 3)], one_recv.at[qb])
        for j in (1, 2, 3, 0):
            tz, tx = lax.rem(z + j, 4), lax.rem(x + j, 4)
            for cc in (c, oc):
                rows = pl.ds(pl.multiple_of(cc * 32, 32), 32)
                if j == 0 and cc is c:
                    out[ea, :, zwide] = relay[qa, z, rows]
                    for s in range(4):
                        at = pl.ds(pl.multiple_of(s * 512 + x * 128, 128), 128)
                        out[eb, :, at] = relay[qb, x, rows, s * 128 : (s + 1) * 128]
                    continue
                other_core = {} if cc is c else {"c": oc}
                remote(
                    relay.at[qa, tz, rows], out.at[ea, :, zwide], two_send, two_recv,
                    {**zdev(j), **other_core} if j else other_core,
                )
                for s in range(4):
                    at = pl.ds(pl.multiple_of(s * 512 + x * 128, 128), 128)
                    remote(
                        relay.at[qb, tx, rows, pl.ds(s * 128, 128)], out.at[eb, :, at], two_send, two_recv,
                        {**xdev(j), **other_core} if j else other_core,
                    )

    place = b * 2 + c
    chip = pl.ds(pl.multiple_of((z * 4 + x) * 128, 128), 128)

    def router_start():
        wait_bytes(swap.at[1, 0], rt_recv.at[0])
        lane = lax.broadcasted_iota(jnp.int32, (HALF, 128), 1)
        own = (lane < 64) == (c == 0)
        part[...] = jnp.where(own, swap[0, c], swap[1, 0]).astype(BF16)
        router[place, :, chip] = part[...]
        for j in (1, 2, 3):
            remote(part, router.at[place, :, chip], rt_send.at[1], rt_recv.at[1], xdev(j))

    def router_z():
        wait_bytes(router.at[place, :, pl.ds(0, 384)], rt_recv.at[1])
        for j in (1, 2, 3):
            remote(
                router.at[place, :, zwide], router.at[place, :, zwide], rt_send.at[2], rt_recv.at[2], zdev(j)
            )

    def router_y():
        wait_bytes(router.at[place, :, pl.ds(0, 1536)], rt_recv.at[2])
        for j in (1, 2, 3):
            remote(
                router.at[place], router.at[place], rt_send.at[3], rt_recv.at[3], {"b": lax.rem(b + j, 4)}
            )

    def router_core():
        wait_bytes(router.at[pl.ds(0, 3)], rt_recv.at[3])
        for j in range(4):
            remote(router.at[2 * j + c], router.at[2 * j + c], rt_send.at[4], rt_recv.at[4], {"c": oc})

    wait_bytes(full.at[lead, mine], core_recv.at[0])
    wait_bytes(stage_two.at[pl.ds(0, 3), lead], sum_recv.at[2])
    finish(lead)
    first_hop(0)
    for (first, n), _, _, me, dev, before, sem in plans:
        at = pl.ds(first, n)
        wait_bytes(stage_one.at[pl.ds(0, 3), at], sum_recv.at[before])
        stage_two[me, at] = (stage_one[0, at] + stage_one[1, at]) + (stage_one[2, at] + stage_one[3, at])
        for j in (1, 2, 3):
            remote(stage_two.at[me, at], stage_two.at[me, at], sum_send.at[sem], sum_recv.at[sem], dev(j))
    router_start()
    for (first, n), _, _, _, _, _, sem in plans:
        at = pl.ds(first, n)
        wait_bytes(stage_two.at[pl.ds(0, 3), at], sum_recv.at[sem])
        finish(at)
    wait_bytes(full.at[pl.ds(2, 6), mine], core_recv.at[1])
    first_hop(1)
    remote(scale, other, sc_send, sc_recv, {"c": oc})
    router_z()
    first_hop(2)
    second_hop(0)

    def step(p, carry):
        first_hop(p)
        second_hop(p - LAG)
        return carry

    step(3, 0)
    wait_bytes(full.at[pl.ds(8, 8), mine], core_recv.at[2])
    lax.fori_loop(4, 6, step, 0)
    router_y()
    lax.fori_loop(6, 8, step, 0)
    wait_bytes(full.at[pl.ds(16, 8), mine], core_recv.at[3])
    lax.fori_loop(8, 10, step, 0)
    router_core()
    lax.fori_loop(10, PAIRS, step, 0)

    wait_bytes(scale, sc_recv)
    wait_bytes(scale, sc_send)
    index = (z * 4 + x) * 2 + c
    turn_by = lax.rem(4 - lax.rem(index, 4), 4) * 32
    column = pl.ds(pl.multiple_of((index // 4) * 128, 128), 128)

    def emit(q, carry):
        row = (q // HALF) * 16 + lax.rem(q, HALF)
        scales[row + c * HALF] = pltpu.roll(scale[q, :, column], turn_by, 1)[:, :32]
        scales[row + oc * HALF] = pltpu.roll(other[q, :, column], turn_by, 1)[:, :32]
        return carry

    lax.fori_loop(0, SLOTS, emit, 0)

    for p in range(PAIRS - LAG, PAIRS):
        second_hop(p)

    wait_bytes(router.at[pl.ds(0, 4)], rt_recv.at[4])
    wait_bytes(swap.at[1, 0], rt_send.at[0])
    wait_bytes(router.at[place, :, pl.ds(0, 384)], rt_send.at[1])
    wait_bytes(router.at[place, :, pl.ds(0, 1536)], rt_send.at[2])
    wait_bytes(router.at[pl.ds(0, 3)], rt_send.at[3])
    wait_bytes(router.at[pl.ds(0, 4)], rt_send.at[4])
    for k, (first, n) in enumerate(CHUNKS):
        wait_bytes(full.at[pl.ds(first, n), mine], core_send.at[k])
    wait_bytes(pair_sum.at[pl.ds(0, 7)], sum_send.at[0])
    wait_bytes(lent_sum.at[rest], sum_send.at[1])
    wait_bytes(stage_two.at[pl.ds(0, 3), lead], sum_send.at[2])
    for (first, n), _, _, _, _, before, sem in plans:
        wait_bytes(stage_one.at[pl.ds(0, 3), pl.ds(first, n)], sum_send.at[before])
        wait_bytes(stage_two.at[pl.ds(0, 3), pl.ds(first, n)], sum_send.at[sem])
    wait_bytes(turned.at[pl.ds(0, SLOTS * 3 // 4)], one_send)
    wait_bytes(out.at[pl.ds(0, 42)], two_send)
    wait_bytes(out.at[pl.ds(0, 42)], two_recv)


def writer(packed, scales, router, *rest):
    results, sem = rest[:-1], rest[-1]
    copies = []
    for t in range(3):
        for k in range(0, 16, 4):
            copies.append((packed.at[pl.ds(16 * t + k, 4)], results[t].at[pl.ds(k, 4)]))
    for t in range(3):
        copies.append((scales.at[pl.ds(16 * t, 16)], results[3 + t]))
    copies.append((router, results[6]))
    copies = [pltpu.make_async_copy(src, dst, sem.at[k]) for k, (src, dst) in enumerate(copies)]
    for copy in copies:
        copy.start()
    for copy in copies:
        copy.wait()


def body(train_gate, train_up, train_down, router_weight, router_gain):
    vmem = pl.BlockSpec(memory_space=pltpu.VMEM)
    hbm = pl.BlockSpec(memory_space=pltpu.HBM)
    dma = pltpu.SemaphoreType.DMA
    chunks = len(CHUNKS)
    sums = (SLOTS, 1, 1024)
    packed, scales, router = pl.pallas_call(
        kernel,
        out_shape=(
            pltpu.VMEM((48, 32, 2048), BF16),
            pltpu.VMEM((48, 1, 32), F32),
            pltpu.VMEM((8, 8, 2048), BF16),
        ),
        in_specs=[hbm] * 5,
        out_specs=(vmem, vmem, vmem),
        scratch_shapes=[
            pltpu.VMEM((SLOTS, 128, 1024), F32),
            pltpu.VMEM((SLOTS, 64, 1024), F32),
            pltpu.VMEM((SLOTS, 4, 4, 64, 128), BF16),
            pltpu.VMEM((SLOTS, 4, 64, 512), BF16),
            pltpu.VMEM(sums, F32),
            pltpu.VMEM(sums, F32),
            pltpu.VMEM(sums, F32),
            pltpu.VMEM((8, 2, 1, 1024), F32),
            pltpu.VMEM((4,) + sums, F32),
            pltpu.VMEM((4,) + sums, F32),
            pltpu.VMEM(sums, F32),
            pltpu.VMEM(sums, F32),
            pltpu.VMEM(sums, F32),
            pltpu.VMEM((2, 2, HALF, 128), F32),
            pltpu.VMEM((HALF, 128), BF16),
            pltpu.VMEM((16, 64), F32),
            pltpu.VMEM((1, 64), F32),
            dma((2 * chunks + 2,)), dma((chunks,)), dma((chunks,)), dma((7,)), dma((7,)),
            dma, dma((SLOTS,)), dma, dma, dma, dma, dma((5,)), dma((5,)),
        ],
        compiler_params=pltpu.CompilerParams(
            collective_id=0, has_side_effects=True, vmem_limit_bytes=56 * 1024 * 1024
        ),
    )(
        *(
            pltpu.with_memory_space_constraint(a, pltpu.HBM)
            for a in (
                train_gate,
                train_up,
                jnp.transpose(train_down, (0, 2, 1)),
                router_weight.T,
                router_gain.reshape(1, 64),
            )
        )
    )
    tensor = jax.ShapeDtypeStruct((16, 32, 2048), BF16)
    column = jax.ShapeDtypeStruct((16, 1, 32), F32)
    ready_gate, ready_up, ready_down, scale_gate, scale_up, scale_down, serve_router = pl.pallas_call(
        writer,
        out_shape=(tensor,) * 3 + (column,) * 3 + (jax.ShapeDtypeStruct((8, 8, 2048), BF16),),
        in_specs=[vmem] * 3,
        out_specs=(hbm,) * 7,
        scratch_shapes=[dma((16,))],
        compiler_params=pltpu.CompilerParams(vmem_limit_bytes=1024 * 1024),
    )(packed, scales, router)
    return (
        jnp.transpose(ready_gate, (0, 2, 1)),
        jnp.transpose(ready_up, (0, 2, 1)),
        ready_down,
        scale_gate.reshape(16, 32),
        scale_up.reshape(16, 32),
        scale_down.reshape(16, 32),
        serve_router.reshape(64, 2048).T,
    )


def solution(mesh):
    split = Mesh(mesh.devices.reshape(mesh.shape["bank"], 4, 4, 2), ("b",) + ZERO)
    return jax.shard_map(
        body,
        mesh=split,
        in_specs=(P("b", ZERO, None), P("b", ZERO, None), P("b", None, ZERO), P(ZERO, "b"), P(ZERO)),
        out_specs=(
            P("b", None, ZERO),
            P("b", None, ZERO),
            P("b", ZERO, None),
            P("b", ZERO),
            P("b", ZERO),
            P("b", ZERO),
            P(),
        ),
        check_vma=False,
    )
```

```python
import functools

import jax
import jax.numpy as jnp
from jax import lax
from jax.experimental import pallas as pl
from jax.experimental.pallas import tpu as pltpu
from jax.sharding import Mesh
from jax.sharding import PartitionSpec as P

ZERO = ("z", "x", "c")
MESH = pl.DeviceIdType.MESH
F32 = jnp.float32
BF16 = jnp.bfloat16
HALF = 8
SLOTS = 3 * HALF
PAIRS = SLOTS // 2
LAG = 2
CHUNKS = ((0, 2), (2, 6), (8, 8), (16, 8))
LEAD = 8
LATER = ((8, 8), (16, 8))


def kernel(
    gate, up, down, weight, gain, out, scales, router,
    full, half, turned, relay, raw, raw_relay, spread, own_sum, lent_sum, got_sum, chip_sum,
    lead_x, lead_z, quarter_one, quarter_two, total, scale, other, inverse, swap, part, weight_in, gain_in,
    load_sem, core_send, core_recv, sum_send, sum_recv, raw_send, raw_recv,
    one_send, one_recv, two_send, two_recv, sc_send, sc_recv, rt_send, rt_recv,
):
    b, z, x, c = (lax.axis_index(n) for n in ("b", "z", "x", "c"))
    oc = 1 - c

    def xdev(k):
        return {"x": lax.rem(x + k, 4)}

    def zdev(k):
        return {"z": lax.rem(z + k, 4)}

    def remote(src, dst, send, recv, dev):
        pltpu.make_async_remote_copy(
            src_ref=src, dst_ref=dst, send_sem=send, recv_sem=recv, device_id=dev, device_id_type=MESH
        ).start()

    def wait_bytes(ref, sem):
        pltpu.make_async_copy(ref, ref, sem).wait()

    barrier = pltpu.get_barrier_semaphore()
    peers = [{"c": oc}]
    for k in (1, 2, 3):
        peers += [xdev(k), zdev(k), {**xdev(k), "c": oc}, {**zdev(k), "c": oc}, {"b": lax.rem(b + k, 4)}]
    for dev in peers:
        pl.semaphore_signal(barrier, inc=1, device_id=dev, device_id_type=MESH)

    sources = (gate, up, down)
    mine = pl.ds(pl.multiple_of(c * 64, 64), 64)

    loads = []
    for k, (first, n) in enumerate(CHUNKS):
        src, at = sources[first // HALF], pl.ds(first, n)
        loads.append((
            pltpu.make_async_copy(
                src.at[pl.ds(c * HALF + first % HALF, n)], full.at[at, mine], load_sem.at[2 * k]
            ),
            pltpu.make_async_copy(
                src.at[pl.ds(oc * HALF + first % HALF, n)], half.at[at], load_sem.at[2 * k + 1]
            ),
        ))
    loads.append((
        pltpu.make_async_copy(weight, weight_in, load_sem.at[2 * len(CHUNKS)]),
        pltpu.make_async_copy(gain, gain_in, load_sem.at[2 * len(CHUNKS) + 1]),
    ))
    for pair in loads:
        for copy in pair:
            copy.start()

    def arrived(k):
        for copy in loads[k]:
            copy.wait()

    def own_sums(k):
        first, n = CHUNKS[k]
        def one(q, carry):
            rows = full[q, mine]
            own_sum[q] = jnp.sum(rows * rows, axis=0, keepdims=True)
            rows = half[q]
            lent_sum[q] = jnp.sum(rows * rows, axis=0, keepdims=True)
            return carry

        lax.fori_loop(first, first + n, one, 0)

    arrived(0)
    own_sums(0)
    arrived(1)
    own_sums(1)
    arrived(2)
    arrived(3)
    pl.semaphore_wait(barrier, len(peers))

    lead, later = pl.ds(0, LEAD), pl.ds(LEAD, SLOTS - LEAD)
    remote(lent_sum.at[lead], got_sum.at[lead], sum_send.at[0], sum_recv.at[0], {"c": oc})
    for k, (first, n) in enumerate(CHUNKS):
        at = pl.ds(first, n)
        remote(half.at[at], full.at[at, mine], core_send.at[k], core_recv.at[k], {"c": oc})
    for copy in loads[-1]:
        copy.wait()
    product = weight_in[...] * gain_in[...]
    swap[0] = jnp.concatenate([product, product], axis=1).reshape(2, HALF, 128)

    xlane = pl.ds(pl.multiple_of(x * 128, 128), 128)
    zlane = pl.ds(pl.multiple_of(z * 128, 128), 128)

    def four(ref, *at):
        return (ref[0, *at] + ref[1, *at]) + (ref[2, *at] + ref[3, *at])

    def to_peers(ref, at, sem, dev):
        for j in (1, 2, 3):
            remote(ref.at[at], ref.at[at], sum_send.at[sem], sum_recv.at[sem], dev(j))

    def scatter():
        for g, ((first, n), me, dev) in enumerate(zip(LATER, (x, z), (xdev, zdev))):
            quarter_one[g, me] = chip_sum[pl.ds(first + 2 * me, 2)]
            for j in (1, 2, 3):
                to = lax.rem(me + j, 4)
                remote(
                    chip_sum.at[pl.ds(first + 2 * to, 2)], quarter_one.at[g, me],
                    sum_send.at[4 + g], sum_recv.at[4 + g], dev(j),
                )

    def across():
        for g, (me, dev) in enumerate(zip((z, x), (zdev, xdev))):
            wait_bytes(quarter_one.at[g, pl.ds(0, 3)], sum_recv.at[4 + g])
            quarter_two[g, me] = four(quarter_one.at[g])
            for j in (1, 2, 3):
                remote(
                    quarter_two.at[g, me], quarter_two.at[g, me], sum_send.at[6 + g], sum_recv.at[6 + g], dev(j)
                )

    def back():
        for g, ((first, n), me, dev) in enumerate(zip(LATER, (x, z), (xdev, zdev))):
            wait_bytes(quarter_two.at[g, pl.ds(0, 3)], sum_recv.at[6 + g])
            at = pl.ds(first + 2 * me, 2)
            total[at] = four(quarter_two.at[g])
            to_peers(total, at, 8 + g, dev)

    def finish(at):
        root = jnp.sqrt(total[at])
        scale[at] = root
        inverse[at] = 1.0 / root

    def turn_raw(q):
        for j in range(8):
            block = full[q, :, j * 128 : (j + 1) * 128]
            raw[q, j // 2, (j % 2) * 2 : (j % 2) * 2 + 2] = block.T.reshape(2, 64, 128)

    def send_raw_z(j):
        remote(raw.at[1, lax.rem(z + j, 4)], raw_relay.at[1, :, :, zlane], raw_send, raw_recv.at[1], zdev(j))

    def normalise_raw():
        for q, place in ((0, lambda k: k * 4 + x), (1, lambda k: z * 4 + k)):
            for j in range(8):
                row = inverse[q, :, j * 128 : (j + 1) * 128]
                spread[2 * j : 2 * j + 2] = jnp.broadcast_to(row, (128, 128)).T.reshape(2, 64, 128)
            wait_bytes(raw_relay.at[q, pl.ds(0, 3)], raw_recv.at[q])
            for k in range(4):
                factor = spread[place(k)]
                for s in range(4):
                    lanes = slice(s * 128, (s + 1) * 128)
                    relay[q, k, :, lanes] = (raw_relay[q, k, :, lanes] * factor).astype(BF16)

    def turn(q):
        for j in range(8):
            lanes = slice(j * 128, (j + 1) * 128)
            block = (full[q, :, lanes] * inverse[q, :, lanes]).astype(BF16)
            turned[q, j // 2, (j % 2) * 2 : (j % 2) * 2 + 2] = block.T.reshape(2, 64, 128)

    zwide = pl.ds(pl.multiple_of(z * 512, 512), 512)

    def first_hop(p):
        qa, qb = 2 * p, 2 * p + 1
        turn(qa)
        for j in (1, 2, 3):
            to = lax.rem(x + j, 4)
            remote(turned.at[qa, :, to], relay.at[qa, :, :, xlane], one_send, one_recv.at[qa], xdev(j))
        turn(qb)
        for j in (1, 2, 3):
            to = lax.rem(z + j, 4)
            remote(turned.at[qb, to], relay.at[qb, :, :, zlane], one_send, one_recv.at[qb], zdev(j))
        relay[qa, :, :, xlane] = turned[qa, :, x]
        relay[qb, :, :, zlane] = turned[qb, z]

    def second_hop(p):
        qa, qb = 2 * p, 2 * p + 1
        ea = (qa // HALF) * 16 + c * HALF + lax.rem(qa, HALF)
        eb = ea + 1
        if isinstance(p, int) and p == 0:
            normalise_raw()
        else:
            wait_bytes(relay.at[qa, pl.ds(0, 3)], one_recv.at[qa])
            wait_bytes(relay.at[qb, pl.ds(0, 3)], one_recv.at[qb])
        for j in (1, 2, 3, 0):
            tz, tx = lax.rem(z + j, 4), lax.rem(x + j, 4)
            for cc in (c, oc):
                rows = pl.ds(pl.multiple_of(cc * 32, 32), 32)
                if j == 0 and cc is c:
                    out[ea, :, zwide] = relay[qa, z, rows]
                    for s in range(4):
                        at = pl.ds(pl.multiple_of(s * 512 + x * 128, 128), 128)
                        out[eb, :, at] = relay[qb, x, rows, s * 128 : (s + 1) * 128]
                    continue
                other_core = {} if cc is c else {"c": oc}
                remote(
                    relay.at[qa, tz, rows], out.at[ea, :, zwide], two_send, two_recv,
                    {**zdev(j), **other_core} if j else other_core,
                )
                for s in range(4):
                    at = pl.ds(pl.multiple_of(s * 512 + x * 128, 128), 128)
                    remote(
                        relay.at[qb, tx, rows, pl.ds(s * 128, 128)], out.at[eb, :, at], two_send, two_recv,
                        {**xdev(j), **other_core} if j else other_core,
                    )

    place = b * 2 + c
    chip = pl.ds(pl.multiple_of((z * 4 + x) * 128, 128), 128)

    def router_start():
        wait_bytes(swap.at[1, 0], rt_recv.at[0])
        lane = lax.broadcasted_iota(jnp.int32, (HALF, 128), 1)
        own = (lane < 64) == (c == 0)
        part[...] = jnp.where(own, swap[0, c], swap[1, 0]).astype(BF16)
        router[place, :, chip] = part[...]
        for j in (1, 2, 3):
            remote(part, router.at[place, :, chip], rt_send.at[1], rt_recv.at[1], xdev(j))

    def router_z():
        wait_bytes(router.at[place, :, pl.ds(0, 384)], rt_recv.at[1])
        for j in (1, 2, 3):
            remote(
                router.at[place, :, zwide], router.at[place, :, zwide], rt_send.at[2], rt_recv.at[2], zdev(j)
            )

    def router_y():
        wait_bytes(router.at[place, :, pl.ds(0, 1536)], rt_recv.at[2])
        for j in (1, 2, 3):
            remote(
                router.at[place], router.at[place], rt_send.at[3], rt_recv.at[3], {"b": lax.rem(b + j, 4)}
            )

    def router_core():
        wait_bytes(router.at[pl.ds(0, 3)], rt_recv.at[3])
        for j in range(4):
            remote(router.at[2 * j + c], router.at[2 * j + c], rt_send.at[4], rt_recv.at[4], {"c": oc})

    wait_bytes(lent_sum.at[lead], sum_recv.at[0])
    lead_x[x] = own_sum[lead] + got_sum[lead]
    to_peers(lead_x, x, 2, xdev)

    wait_bytes(full.at[pl.ds(0, 2), mine], core_recv.at[0])
    turn_raw(0)
    for j in (1, 2, 3):
        remote(
            raw.at[0, :, lax.rem(x + j, 4)], raw_relay.at[0, :, :, xlane], raw_send, raw_recv.at[0], xdev(j)
        )
    turn_raw(1)
    send_raw_z(1)
    send_raw_z(3)
    raw_relay[0, :, :, xlane] = raw[0, :, x]
    raw_relay[1, :, :, zlane] = raw[1, z]

    own_sums(2)
    own_sums(3)
    remote(lent_sum.at[later], got_sum.at[later], sum_send.at[1], sum_recv.at[1], {"c": oc})
    wait_bytes(lead_x.at[pl.ds(0, 3)], sum_recv.at[2])
    lead_z[z] = four(lead_x)
    to_peers(lead_z, z, 3, zdev)
    send_raw_z(2)
    wait_bytes(lent_sum.at[later], sum_recv.at[1])
    chip_sum[later] = own_sum[later] + got_sum[later]
    scatter()
    remote(swap.at[0, oc], swap.at[1, 0], rt_send.at[0], rt_recv.at[0], {"c": oc})
    wait_bytes(lead_z.at[pl.ds(0, 3)], sum_recv.at[3])
    total[lead] = four(lead_z)
    finish(lead)
    wait_bytes(full.at[pl.ds(2, 6), mine], core_recv.at[1])
    first_hop(1)
    first_hop(2)
    across()
    second_hop(0)
    back()
    router_start()
    first_hop(3)
    second_hop(1)
    router_z()
    for g, (first, n) in enumerate(LATER):
        wait_bytes(total.at[pl.ds(first, 6)], sum_recv.at[8 + g])
    finish(later)
    remote(scale, other, sc_send, sc_recv, {"c": oc})

    def step(p, carry):
        first_hop(p)
        second_hop(p - LAG)
        return carry

    wait_bytes(full.at[pl.ds(8, 8), mine], core_recv.at[2])
    lax.fori_loop(4, 6, step, 0)
    router_y()
    lax.fori_loop(6, 8, step, 0)
    wait_bytes(full.at[pl.ds(16, 8), mine], core_recv.at[3])
    lax.fori_loop(8, 10, step, 0)
    router_core()
    lax.fori_loop(10, PAIRS, step, 0)

    wait_bytes(scale, sc_recv)
    wait_bytes(scale, sc_send)
    index = (z * 4 + x) * 2 + c
    turn_by = lax.rem(4 - lax.rem(index, 4), 4) * 32
    column = pl.ds(pl.multiple_of((index // 4) * 128, 128), 128)

    def emit(q, carry):
        row = (q // HALF) * 16 + lax.rem(q, HALF)
        scales[row + c * HALF] = pltpu.roll(scale[q, :, column], turn_by, 1)[:, :32]
        scales[row + oc * HALF] = pltpu.roll(other[q, :, column], turn_by, 1)[:, :32]
        return carry

    lax.fori_loop(0, SLOTS, emit, 0)

    for p in range(PAIRS - LAG, PAIRS):
        second_hop(p)

    wait_bytes(router.at[pl.ds(0, 4)], rt_recv.at[4])
    wait_bytes(swap.at[1, 0], rt_send.at[0])
    wait_bytes(router.at[place, :, pl.ds(0, 384)], rt_send.at[1])
    wait_bytes(router.at[place, :, pl.ds(0, 1536)], rt_send.at[2])
    wait_bytes(router.at[pl.ds(0, 3)], rt_send.at[3])
    wait_bytes(router.at[pl.ds(0, 4)], rt_send.at[4])
    for k, (first, n) in enumerate(CHUNKS):
        wait_bytes(full.at[pl.ds(first, n), mine], core_send.at[k])
    wait_bytes(lent_sum.at[lead], sum_send.at[0])
    wait_bytes(lent_sum.at[later], sum_send.at[1])
    wait_bytes(lead_x.at[pl.ds(0, 3)], sum_send.at[2])
    wait_bytes(lead_z.at[pl.ds(0, 3)], sum_send.at[3])
    for k in range(6):
        wait_bytes(total.at[pl.ds(0, 6)], sum_send.at[4 + k])
    wait_bytes(raw.at[:, pl.ds(0, 3)], raw_send)
    wait_bytes(turned.at[pl.ds(0, SLOTS - 2), pl.ds(0, 3)], one_send)
    wait_bytes(out.at[pl.ds(0, 42)], two_send)
    wait_bytes(out.at[pl.ds(0, 42)], two_recv)


def writer(packed, scales, router, *rest):
    results, sem = rest[:-1], rest[-1]
    copies = []
    for t in range(3):
        for k in range(0, 16, 4):
            copies.append((packed.at[pl.ds(16 * t + k, 4)], results[t].at[pl.ds(k, 4)]))
    for t in range(3):
        copies.append((scales.at[pl.ds(16 * t, 16)], results[3 + t]))
    copies.append((router, results[6]))
    copies = [pltpu.make_async_copy(src, dst, sem.at[k]) for k, (src, dst) in enumerate(copies)]
    for copy in copies:
        copy.start()
    for copy in copies:
        copy.wait()


def body(train_gate, train_up, train_down, router_weight, router_gain):
    vmem = pl.BlockSpec(memory_space=pltpu.VMEM)
    hbm = pl.BlockSpec(memory_space=pltpu.HBM)
    dma = pltpu.SemaphoreType.DMA
    chunks = len(CHUNKS)
    sums = (SLOTS, 1, 1024)
    packed, scales, router = pl.pallas_call(
        kernel,
        out_shape=(
            pltpu.VMEM((48, 32, 2048), BF16),
            pltpu.VMEM((48, 1, 32), F32),
            pltpu.VMEM((8, 8, 2048), BF16),
        ),
        in_specs=[hbm] * 5,
        out_specs=(vmem, vmem, vmem),
        scratch_shapes=[
            pltpu.VMEM((SLOTS, 128, 1024), F32),
            pltpu.VMEM((SLOTS, 64, 1024), F32),
            pltpu.VMEM((SLOTS, 4, 4, 64, 128), BF16),
            pltpu.VMEM((SLOTS, 4, 64, 512), BF16),
            pltpu.VMEM((2, 4, 4, 64, 128), F32),
            pltpu.VMEM((2, 4, 64, 512), F32),
            pltpu.VMEM((16, 64, 128), F32),
            pltpu.VMEM(sums, F32),
            pltpu.VMEM(sums, F32),
            pltpu.VMEM(sums, F32),
            pltpu.VMEM(sums, F32),
            pltpu.VMEM((4, LEAD, 1, 1024), F32),
            pltpu.VMEM((4, LEAD, 1, 1024), F32),
            pltpu.VMEM((2, 4, 2, 1, 1024), F32),
            pltpu.VMEM((2, 4, 2, 1, 1024), F32),
            pltpu.VMEM(sums, F32),
            pltpu.VMEM(sums, F32),
            pltpu.VMEM(sums, F32),
            pltpu.VMEM(sums, F32),
            pltpu.VMEM((2, 2, HALF, 128), F32),
            pltpu.VMEM((HALF, 128), BF16),
            pltpu.VMEM((16, 64), F32),
            pltpu.VMEM((1, 64), F32),
            dma((2 * chunks + 2,)), dma((chunks,)), dma((chunks,)), dma((10,)), dma((10,)), dma, dma((2,)),
            dma, dma((SLOTS,)), dma, dma, dma, dma, dma((5,)), dma((5,)),
        ],
        compiler_params=pltpu.CompilerParams(
            collective_id=0, has_side_effects=True, vmem_limit_bytes=56 * 1024 * 1024
        ),
    )(
        *(
            pltpu.with_memory_space_constraint(a, pltpu.HBM)
            for a in (
                train_gate,
                train_up,
                jnp.transpose(train_down, (0, 2, 1)),
                router_weight.T,
                router_gain.reshape(1, 64),
            )
        )
    )
    tensor = jax.ShapeDtypeStruct((16, 32, 2048), BF16)
    column = jax.ShapeDtypeStruct((16, 1, 32), F32)
    ready_gate, ready_up, ready_down, scale_gate, scale_up, scale_down, serve_router = pl.pallas_call(
        writer,
        out_shape=(tensor,) * 3 + (column,) * 3 + (jax.ShapeDtypeStruct((8, 8, 2048), BF16),),
        in_specs=[vmem] * 3,
        out_specs=(hbm,) * 7,
        scratch_shapes=[dma((16,))],
        compiler_params=pltpu.CompilerParams(vmem_limit_bytes=1024 * 1024),
    )(packed, scales, router)
    return (
        jnp.transpose(ready_gate, (0, 2, 1)),
        jnp.transpose(ready_up, (0, 2, 1)),
        ready_down,
        scale_gate.reshape(16, 32),
        scale_up.reshape(16, 32),
        scale_down.reshape(16, 32),
        serve_router.reshape(64, 2048).T,
    )


def solution(mesh):
    split = Mesh(mesh.devices.reshape(mesh.shape["bank"], 4, 4, 2), ("b",) + ZERO)
    return jax.shard_map(
        body,
        mesh=split,
        in_specs=(P("b", ZERO, None), P("b", ZERO, None), P("b", None, ZERO), P(ZERO, "b"), P(ZERO)),
        out_specs=(
            P("b", None, ZERO),
            P("b", None, ZERO),
            P("b", ZERO, None),
            P("b", ZERO),
            P("b", ZERO),
            P("b", ZERO),
            P(),
        ),
        check_vma=False,
    )
```

```python
import functools

import jax
import jax.numpy as jnp
from jax import lax
from jax.experimental import pallas as pl
from jax.experimental.pallas import tpu as pltpu
from jax.sharding import Mesh
from jax.sharding import PartitionSpec as P

ZERO = ("z", "x", "c")
MESH = pl.DeviceIdType.MESH
F32 = jnp.float32
BF16 = jnp.bfloat16
HALF = 8
SLOTS = 3 * HALF
PAIRS = SLOTS // 2
LAG = 2
CHUNKS = ((0, 2), (2, 6), (8, 8), (16, 8))
LEAD = 8
LATER = ((8, 8), (16, 8))


def kernel(
    gate, up, down, weight, gain, out, scales, router,
    full, half, turned, relay, raw, raw_relay, spread, own_sum, lent_sum, got_sum, chip_sum,
    lead_x, lead_z, quarter_one, quarter_two, total, scale, other, inverse, swap, part, weight_in, gain_in,
    load_sem, core_send, core_recv, sum_send, sum_recv, raw_send, raw_recv,
    one_send, one_recv, two_send, two_recv, sc_send, sc_recv, rt_send, rt_recv,
):
    b, z, x, c = (lax.axis_index(n) for n in ("b", "z", "x", "c"))
    oc = 1 - c

    def xdev(k):
        return {"x": lax.rem(x + k, 4)}

    def zdev(k):
        return {"z": lax.rem(z + k, 4)}

    def remote(src, dst, send, recv, dev):
        pltpu.make_async_remote_copy(
            src_ref=src, dst_ref=dst, send_sem=send, recv_sem=recv, device_id=dev, device_id_type=MESH
        ).start()

    def wait_bytes(ref, sem):
        pltpu.make_async_copy(ref, ref, sem).wait()

    barrier = pltpu.get_barrier_semaphore()
    peers = [{"c": oc}]
    for k in (1, 2, 3):
        peers += [xdev(k), zdev(k), {**xdev(k), "c": oc}, {**zdev(k), "c": oc}, {"b": lax.rem(b + k, 4)}]
    for dev in peers:
        pl.semaphore_signal(barrier, inc=1, device_id=dev, device_id_type=MESH)

    sources = (gate, up, down)
    mine = pl.ds(pl.multiple_of(c * 64, 64), 64)

    loads = []
    for k, (first, n) in enumerate(CHUNKS):
        src, at = sources[first // HALF], pl.ds(first, n)
        loads.append((
            pltpu.make_async_copy(
                src.at[pl.ds(c * HALF + first % HALF, n)], full.at[at, mine], load_sem.at[2 * k]
            ),
            pltpu.make_async_copy(
                src.at[pl.ds(oc * HALF + first % HALF, n)], half.at[at], load_sem.at[2 * k + 1]
            ),
        ))
    loads.append((
        pltpu.make_async_copy(weight, weight_in, load_sem.at[2 * len(CHUNKS)]),
        pltpu.make_async_copy(gain, gain_in, load_sem.at[2 * len(CHUNKS) + 1]),
    ))
    for pair in (loads[0], loads[1]):
        for copy in pair:
            copy.start()

    def arrived(k):
        for copy in loads[k]:
            copy.wait()

    def own_sums(k):
        first, n = CHUNKS[k]
        def one(q, carry):
            rows = full[q, mine]
            own_sum[q] = jnp.sum(rows * rows, axis=0, keepdims=True)
            rows = half[q]
            lent_sum[q] = jnp.sum(rows * rows, axis=0, keepdims=True)
            return carry

        lax.fori_loop(first, first + n, one, 0)

    arrived(0)
    for pair in loads[2:]:
        for copy in pair:
            copy.start()
    own_sums(0)
    arrived(1)
    own_sums(1)
    pl.semaphore_wait(barrier, len(peers))

    lead, later = pl.ds(0, LEAD), pl.ds(LEAD, SLOTS - LEAD)
    remote(lent_sum.at[lead], got_sum.at[lead], sum_send.at[0], sum_recv.at[0], {"c": oc})

    def lend(k):
        first, n = CHUNKS[k]
        at = pl.ds(first, n)
        remote(half.at[at], full.at[at, mine], core_send.at[k], core_recv.at[k], {"c": oc})

    lend(0)
    lend(1)
    for copy in loads[-1]:
        copy.wait()
    product = weight_in[...] * gain_in[...]
    swap[0] = jnp.concatenate([product, product], axis=1).reshape(2, HALF, 128)

    xlane = pl.ds(pl.multiple_of(x * 128, 128), 128)
    zlane = pl.ds(pl.multiple_of(z * 128, 128), 128)

    def four(ref, *at):
        return (ref[0, *at] + ref[1, *at]) + (ref[2, *at] + ref[3, *at])

    def to_peers(ref, at, sem, dev):
        for j in (1, 2, 3):
            remote(ref.at[at], ref.at[at], sum_send.at[sem], sum_recv.at[sem], dev(j))

    def scatter():
        for g, ((first, n), me, dev) in enumerate(zip(LATER, (x, z), (xdev, zdev))):
            quarter_one[g, me] = chip_sum[pl.ds(first + 2 * me, 2)]
            for j in (1, 2, 3):
                to = lax.rem(me + j, 4)
                remote(
                    chip_sum.at[pl.ds(first + 2 * to, 2)], quarter_one.at[g, me],
                    sum_send.at[4 + g], sum_recv.at[4 + g], dev(j),
                )

    def across():
        for g, (me, dev) in enumerate(zip((z, x), (zdev, xdev))):
            wait_bytes(quarter_one.at[g, pl.ds(0, 3)], sum_recv.at[4 + g])
            quarter_two[g, me] = four(quarter_one.at[g])
            for j in (1, 2, 3):
                remote(
                    quarter_two.at[g, me], quarter_two.at[g, me], sum_send.at[6 + g], sum_recv.at[6 + g], dev(j)
                )

    def back():
        for g, ((first, n), me, dev) in enumerate(zip(LATER, (x, z), (xdev, zdev))):
            wait_bytes(quarter_two.at[g, pl.ds(0, 3)], sum_recv.at[6 + g])
            at = pl.ds(first + 2 * me, 2)
            total[at] = four(quarter_two.at[g])
            to_peers(total, at, 8 + g, dev)

    def finish(at):
        root = jnp.sqrt(total[at])
        scale[at] = root
        inverse[at] = 1.0 / root

    def turn_raw(q):
        for j in range(8):
            block = full[q, :, j * 128 : (j + 1) * 128]
            raw[q, j // 2, (j % 2) * 2 : (j % 2) * 2 + 2] = block.T.reshape(2, 64, 128)

    def send_raw_z(j):
        remote(raw.at[1, lax.rem(z + j, 4)], raw_relay.at[1, :, :, zlane], raw_send, raw_recv.at[1], zdev(j))

    def normalise_raw():
        for q, place in ((0, lambda k: k * 4 + x), (1, lambda k: z * 4 + k)):
            for j in range(8):
                row = inverse[q, :, j * 128 : (j + 1) * 128]
                spread[2 * j : 2 * j + 2] = jnp.broadcast_to(row, (128, 128)).T.reshape(2, 64, 128)
            wait_bytes(raw_relay.at[q, pl.ds(0, 3)], raw_recv.at[q])
            for k in range(4):
                factor = spread[place(k)]
                for s in range(4):
                    lanes = slice(s * 128, (s + 1) * 128)
                    relay[q, k, :, lanes] = (raw_relay[q, k, :, lanes] * factor).astype(BF16)

    def turn(q):
        for j in range(8):
            lanes = slice(j * 128, (j + 1) * 128)
            block = (full[q, :, lanes] * inverse[q, :, lanes]).astype(BF16)
            turned[q, j // 2, (j % 2) * 2 : (j % 2) * 2 + 2] = block.T.reshape(2, 64, 128)

    zwide = pl.ds(pl.multiple_of(z * 512, 512), 512)

    def first_hop(p):
        qa, qb = 2 * p, 2 * p + 1
        turn(qa)
        for j in (1, 2, 3):
            to = lax.rem(x + j, 4)
            remote(turned.at[qa, :, to], relay.at[qa, :, :, xlane], one_send, one_recv.at[qa], xdev(j))
        turn(qb)
        for j in (1, 2, 3):
            to = lax.rem(z + j, 4)
            remote(turned.at[qb, to], relay.at[qb, :, :, zlane], one_send, one_recv.at[qb], zdev(j))
        relay[qa, :, :, xlane] = turned[qa, :, x]
        relay[qb, :, :, zlane] = turned[qb, z]

    def second_hop(p):
        qa, qb = 2 * p, 2 * p + 1
        ea = (qa // HALF) * 16 + c * HALF + lax.rem(qa, HALF)
        eb = ea + 1
        if isinstance(p, int) and p == 0:
            normalise_raw()
        else:
            wait_bytes(relay.at[qa, pl.ds(0, 3)], one_recv.at[qa])
            wait_bytes(relay.at[qb, pl.ds(0, 3)], one_recv.at[qb])
        for j in (1, 2, 3, 0):
            tz, tx = lax.rem(z + j, 4), lax.rem(x + j, 4)
            for cc in (c, oc):
                rows = pl.ds(pl.multiple_of(cc * 32, 32), 32)
                if j == 0 and cc is c:
                    out[ea, :, zwide] = relay[qa, z, rows]
                    for s in range(4):
                        at = pl.ds(pl.multiple_of(s * 512 + x * 128, 128), 128)
                        out[eb, :, at] = relay[qb, x, rows, s * 128 : (s + 1) * 128]
                    continue
                other_core = {} if cc is c else {"c": oc}
                remote(
                    relay.at[qa, tz, rows], out.at[ea, :, zwide], two_send, two_recv,
                    {**zdev(j), **other_core} if j else other_core,
                )
                for s in range(4):
                    at = pl.ds(pl.multiple_of(s * 512 + x * 128, 128), 128)
                    remote(
                        relay.at[qb, tx, rows, pl.ds(s * 128, 128)], out.at[eb, :, at], two_send, two_recv,
                        {**xdev(j), **other_core} if j else other_core,
                    )

    place = b * 2 + c
    chip = pl.ds(pl.multiple_of((z * 4 + x) * 128, 128), 128)

    def router_start():
        wait_bytes(swap.at[1, 0], rt_recv.at[0])
        lane = lax.broadcasted_iota(jnp.int32, (HALF, 128), 1)
        own = (lane < 64) == (c == 0)
        part[...] = jnp.where(own, swap[0, c], swap[1, 0]).astype(BF16)
        router[place, :, chip] = part[...]
        for j in (1, 2, 3):
            remote(part, router.at[place, :, chip], rt_send.at[1], rt_recv.at[1], xdev(j))

    def router_z():
        wait_bytes(router.at[place, :, pl.ds(0, 384)], rt_recv.at[1])
        for j in (1, 2, 3):
            remote(
                router.at[place, :, zwide], router.at[place, :, zwide], rt_send.at[2], rt_recv.at[2], zdev(j)
            )

    def router_y():
        wait_bytes(router.at[place, :, pl.ds(0, 1536)], rt_recv.at[2])
        for j in (1, 2, 3):
            remote(
                router.at[place], router.at[place], rt_send.at[3], rt_recv.at[3], {"b": lax.rem(b + j, 4)}
            )

    def router_core():
        wait_bytes(router.at[pl.ds(0, 3)], rt_recv.at[3])
        for j in range(4):
            remote(router.at[2 * j + c], router.at[2 * j + c], rt_send.at[4], rt_recv.at[4], {"c": oc})

    wait_bytes(lent_sum.at[lead], sum_recv.at[0])
    lead_x[x] = own_sum[lead] + got_sum[lead]
    to_peers(lead_x, x, 2, xdev)

    wait_bytes(full.at[pl.ds(0, 2), mine], core_recv.at[0])
    turn_raw(0)
    for j in (1, 2, 3):
        remote(
            raw.at[0, :, lax.rem(x + j, 4)], raw_relay.at[0, :, :, xlane], raw_send, raw_recv.at[0], xdev(j)
        )
    turn_raw(1)
    send_raw_z(1)
    send_raw_z(3)
    raw_relay[0, :, :, xlane] = raw[0, :, x]
    raw_relay[1, :, :, zlane] = raw[1, z]

    arrived(2)
    lend(2)
    arrived(3)
    lend(3)
    own_sums(2)
    own_sums(3)
    remote(lent_sum.at[later], got_sum.at[later], sum_send.at[1], sum_recv.at[1], {"c": oc})
    wait_bytes(lead_x.at[pl.ds(0, 3)], sum_recv.at[2])
    lead_z[z] = four(lead_x)
    to_peers(lead_z, z, 3, zdev)
    send_raw_z(2)
    wait_bytes(lent_sum.at[later], sum_recv.at[1])
    chip_sum[later] = own_sum[later] + got_sum[later]
    scatter()
    remote(swap.at[0, oc], swap.at[1, 0], rt_send.at[0], rt_recv.at[0], {"c": oc})
    wait_bytes(lead_z.at[pl.ds(0, 3)], sum_recv.at[3])
    total[lead] = four(lead_z)
    finish(lead)
    wait_bytes(full.at[pl.ds(2, 6), mine], core_recv.at[1])
    first_hop(1)
    first_hop(2)
    across()
    second_hop(0)
    back()
    router_start()
    first_hop(3)
    second_hop(1)
    router_z()
    for g, (first, n) in enumerate(LATER):
        wait_bytes(total.at[pl.ds(first, 6)], sum_recv.at[8 + g])
    finish(later)
    remote(scale, other, sc_send, sc_recv, {"c": oc})

    def step(p, carry):
        first_hop(p)
        second_hop(p - LAG)
        return carry

    wait_bytes(full.at[pl.ds(8, 8), mine], core_recv.at[2])
    lax.fori_loop(4, 6, step, 0)
    router_y()
    lax.fori_loop(6, 8, step, 0)
    wait_bytes(full.at[pl.ds(16, 8), mine], core_recv.at[3])
    lax.fori_loop(8, 10, step, 0)
    router_core()
    lax.fori_loop(10, PAIRS, step, 0)

    wait_bytes(scale, sc_recv)
    wait_bytes(scale, sc_send)
    index = (z * 4 + x) * 2 + c
    turn_by = lax.rem(4 - lax.rem(index, 4), 4) * 32
    column = pl.ds(pl.multiple_of((index // 4) * 128, 128), 128)

    def emit(q, carry):
        row = (q // HALF) * 16 + lax.rem(q, HALF)
        scales[row + c * HALF] = pltpu.roll(scale[q, :, column], turn_by, 1)[:, :32]
        scales[row + oc * HALF] = pltpu.roll(other[q, :, column], turn_by, 1)[:, :32]
        return carry

    lax.fori_loop(0, SLOTS, emit, 0)

    for p in range(PAIRS - LAG, PAIRS):
        second_hop(p)

    wait_bytes(router.at[pl.ds(0, 4)], rt_recv.at[4])
    wait_bytes(swap.at[1, 0], rt_send.at[0])
    wait_bytes(router.at[place, :, pl.ds(0, 384)], rt_send.at[1])
    wait_bytes(router.at[place, :, pl.ds(0, 1536)], rt_send.at[2])
    wait_bytes(router.at[pl.ds(0, 3)], rt_send.at[3])
    wait_bytes(router.at[pl.ds(0, 4)], rt_send.at[4])
    for k, (first, n) in enumerate(CHUNKS):
        wait_bytes(full.at[pl.ds(first, n), mine], core_send.at[k])
    wait_bytes(lent_sum.at[lead], sum_send.at[0])
    wait_bytes(lent_sum.at[later], sum_send.at[1])
    wait_bytes(lead_x.at[pl.ds(0, 3)], sum_send.at[2])
    wait_bytes(lead_z.at[pl.ds(0, 3)], sum_send.at[3])
    for k in range(6):
        wait_bytes(total.at[pl.ds(0, 6)], sum_send.at[4 + k])
    wait_bytes(raw.at[:, pl.ds(0, 3)], raw_send)
    wait_bytes(turned.at[pl.ds(0, SLOTS - 2), pl.ds(0, 3)], one_send)
    wait_bytes(out.at[pl.ds(0, 42)], two_send)
    wait_bytes(out.at[pl.ds(0, 42)], two_recv)


def writer(packed, scales, router, *rest):
    results, sem = rest[:-1], rest[-1]
    copies = []
    for t in range(3):
        for k in range(0, 16, 4):
            copies.append((packed.at[pl.ds(16 * t + k, 4)], results[t].at[pl.ds(k, 4)]))
    for t in range(3):
        copies.append((scales.at[pl.ds(16 * t, 16)], results[3 + t]))
    copies.append((router, results[6]))
    copies = [pltpu.make_async_copy(src, dst, sem.at[k]) for k, (src, dst) in enumerate(copies)]
    for copy in copies:
        copy.start()
    for copy in copies:
        copy.wait()


def body(train_gate, train_up, train_down, router_weight, router_gain):
    vmem = pl.BlockSpec(memory_space=pltpu.VMEM)
    hbm = pl.BlockSpec(memory_space=pltpu.HBM)
    dma = pltpu.SemaphoreType.DMA
    chunks = len(CHUNKS)
    sums = (SLOTS, 1, 1024)
    packed, scales, router = pl.pallas_call(
        kernel,
        out_shape=(
            pltpu.VMEM((48, 32, 2048), BF16),
            pltpu.VMEM((48, 1, 32), F32),
            pltpu.VMEM((8, 8, 2048), BF16),
        ),
        in_specs=[hbm] * 5,
        out_specs=(vmem, vmem, vmem),
        scratch_shapes=[
            pltpu.VMEM((SLOTS, 128, 1024), F32),
            pltpu.VMEM((SLOTS, 64, 1024), F32),
            pltpu.VMEM((SLOTS, 4, 4, 64, 128), BF16),
            pltpu.VMEM((SLOTS, 4, 64, 512), BF16),
            pltpu.VMEM((2, 4, 4, 64, 128), F32),
            pltpu.VMEM((2, 4, 64, 512), F32),
            pltpu.VMEM((16, 64, 128), F32),
            pltpu.VMEM(sums, F32),
            pltpu.VMEM(sums, F32),
            pltpu.VMEM(sums, F32),
            pltpu.VMEM(sums, F32),
            pltpu.VMEM((4, LEAD, 1, 1024), F32),
            pltpu.VMEM((4, LEAD, 1, 1024), F32),
            pltpu.VMEM((2, 4, 2, 1, 1024), F32),
            pltpu.VMEM((2, 4, 2, 1, 1024), F32),
            pltpu.VMEM(sums, F32),
            pltpu.VMEM(sums, F32),
            pltpu.VMEM(sums, F32),
            pltpu.VMEM(sums, F32),
            pltpu.VMEM((2, 2, HALF, 128), F32),
            pltpu.VMEM((HALF, 128), BF16),
            pltpu.VMEM((16, 64), F32),
            pltpu.VMEM((1, 64), F32),
            dma((2 * chunks + 2,)), dma((chunks,)), dma((chunks,)), dma((10,)), dma((10,)), dma, dma((2,)),
            dma, dma((SLOTS,)), dma, dma, dma, dma, dma((5,)), dma((5,)),
        ],
        compiler_params=pltpu.CompilerParams(
            collective_id=0, has_side_effects=True, vmem_limit_bytes=56 * 1024 * 1024
        ),
    )(
        *(
            pltpu.with_memory_space_constraint(a, pltpu.HBM)
            for a in (
                train_gate,
                train_up,
                jnp.transpose(train_down, (0, 2, 1)),
                router_weight.T,
                router_gain.reshape(1, 64),
            )
        )
    )
    tensor = jax.ShapeDtypeStruct((16, 32, 2048), BF16)
    column = jax.ShapeDtypeStruct((16, 1, 32), F32)
    ready_gate, ready_up, ready_down, scale_gate, scale_up, scale_down, serve_router = pl.pallas_call(
        writer,
        out_shape=(tensor,) * 3 + (column,) * 3 + (jax.ShapeDtypeStruct((8, 8, 2048), BF16),),
        in_specs=[vmem] * 3,
        out_specs=(hbm,) * 7,
        scratch_shapes=[dma((16,))],
        compiler_params=pltpu.CompilerParams(vmem_limit_bytes=1024 * 1024),
    )(packed, scales, router)
    return (
        jnp.transpose(ready_gate, (0, 2, 1)),
        jnp.transpose(ready_up, (0, 2, 1)),
        ready_down,
        scale_gate.reshape(16, 32),
        scale_up.reshape(16, 32),
        scale_down.reshape(16, 32),
        serve_router.reshape(64, 2048).T,
    )


def solution(mesh):
    split = Mesh(mesh.devices.reshape(mesh.shape["bank"], 4, 4, 2), ("b",) + ZERO)
    return jax.shard_map(
        body,
        mesh=split,
        in_specs=(P("b", ZERO, None), P("b", ZERO, None), P("b", None, ZERO), P(ZERO, "b"), P(ZERO)),
        out_specs=(
            P("b", None, ZERO),
            P("b", None, ZERO),
            P("b", ZERO, None),
            P("b", ZERO),
            P("b", ZERO),
            P("b", ZERO),
            P(),
        ),
        check_vma=False,
    )
```
